32 devices in a mesh: dp: 8 (over y, x, core), tensor: 4 (over z).
Axes of the slice: x: 2, y: 2, z: 4, core: 2. Of those that a mesh axis runs over, the one named last changes fastest.
Arguments:
- layer_input: bfloat16 [12288, 2048], P('dp'), may hold values from -30 to 30
- cotangent: bfloat16 [12288, 2048], P('dp'), may hold values from -6 to 6
- lengths: int32 [24], P('dp'), may hold values from 0 to 512, as said below
- projector: float32 [2048, 6144], P('dp', 'tensor'), may hold values from -0.125 to 0.125
- projector_moments: float32 [2, 2048, 6144], P(None, 'dp', 'tensor'), as said below
- shifts: float32 [8, 768], P('tensor', 'dp'), may hold values from -3 to 3
- shifts_moments: float32 [2, 8, 768], P(None, 'tensor', 'dp'), as said below
- combiner: float32 [2048, 2048], P('tensor', 'dp'), may hold values from -1.5 to 1.5
- combiner_moments: float32 [2, 2048, 2048], P(None, 'tensor', 'dp'), as said below
- expander: float32 [2048, 8192], P('dp', 'tensor'), may hold values from -0.125 to 0.125
- expander_moments: float32 [2, 2048, 8192], P(None, 'dp', 'tensor'), as said below
- offsets: float32 [8, 1024], P('tensor', 'dp'), may hold values from -3 to 3
- offsets_moments: float32 [2, 8, 1024], P(None, 'tensor', 'dp'), as said below
- reducer: float32 [8192, 2048], P('tensor', 'dp'), may hold values from -0.0625 to 0.0625
- reducer_moments: float32 [2, 8192, 2048], P(None, 'tensor', 'dp'), as said below
- vectors: float32 [6, 2048], P(None, ('dp', 'tensor')), may hold values from -2 to 2
- vectors_moments: float32 [2, 6, 2048], P(None, None, ('dp', 'tensor')), as said below
Outputs:
- layer_output: bfloat16 [12288, 2048], P('dp', 'tensor')
- input_gradient: bfloat16 [12288, 2048], P('dp', 'tensor')
- projector_gradient: float32 [2048, 6144], P('dp', 'tensor')
- projector_states: float32 [2, 2048, 6144], P(None, 'dp', 'tensor')
- projector_update: float32 [2048, 6144], P('dp', 'tensor')
- shifts_gradient: float32 [8, 768], P('tensor', 'dp')
- shifts_states: float32 [2, 8, 768], P(None, 'tensor', 'dp')
- shifts_update: float32 [8, 768], P('tensor', 'dp')
- combiner_gradient: float32 [2048, 2048], P('tensor', 'dp')
- combiner_states: float32 [2, 2048, 2048], P(None, 'tensor', 'dp')
- combiner_update: float32 [2048, 2048], P('tensor', 'dp')
- expander_gradient: float32 [2048, 8192], P('dp', 'tensor')
- expander_states: float32 [2, 2048, 8192], P(None, 'dp', 'tensor')
- expander_update: float32 [2048, 8192], P('dp', 'tensor')
- offsets_gradient: float32 [8, 1024], P('tensor', 'dp')
- offsets_states: float32 [2, 8, 1024], P(None, 'tensor', 'dp')
- offsets_update: float32 [8, 1024], P('tensor', 'dp')
- reducer_gradient: float32 [8192, 2048], P('tensor', 'dp')
- reducer_states: float32 [2, 8192, 2048], P(None, 'tensor', 'dp')
- reducer_update: float32 [8192, 2048], P('tensor', 'dp')
- vectors_gradient: float32 [6, 2048], P(None, ('dp', 'tensor'))
- vectors_states: float32 [2, 6, 2048], P(None, None, ('dp', 'tensor'))
- vectors_update: float32 [6, 2048], P(None, ('dp', 'tensor'))
The draws below stay inside these ranges and needn't reach their ends.
Inputs may be any that keep to these rules, and one draw needn't show every extreme that they name: `lengths`: dp index i holds slots i * 3 to i * 3 + 2; a slot is empty (0) or holds one sequence of 128 to 512 tokens; every index holds at least one sequence, some index has all its slots filled, one of them with 512 tokens, and some index holds exactly one sequence. `projector_moments`: the roots of the second moments (index 1 of the first dimension) are positive. `shifts_moments`: the roots of the second moments are positive. `combiner_moments`: the roots of the second moments are positive. `expander_moments`: the roots of the second moments are positive. `offsets_moments`: the roots of the second moments are positive. `reducer_moments`: the roots of the second moments are positive. `vectors_moments`: the roots of the second moments are positive.
All inputs are finite; a program needn't handle non-finite values.
Results may differ from the reference program's by a relative error of at most 0.014.
The reference program's roundings to bfloat16 on the way count: a program that leaves them out, or rounds other values in their place, can miss the bound.
Values may be sent and summed in bfloat16 or wider, within the bound.
A program may use at most 320 MiB of HBM per device.

```python
import math
from functools import partial
import jax
import jax.numpy as jnp
from jax import lax

D = 2048
HEADS = 8
HD = 256
ROT = 64
FF = 8192
SEQ_LEN = 512
SEQ_DEV = 3
STEP = 10
SEQS = 24
TOKENS = 12288


def draw_lengths(key, part):
    subkeys = jax.random.split(key, 5)
    devices = SEQS // SEQ_DEV
    counts = jax.random.randint(subkeys[0], (devices,), max(1, SEQ_DEV - 1), SEQ_DEV + 1)
    fullest = jax.random.randint(subkeys[1], (), 0, devices)
    lightest = (fullest + 1 + jax.random.randint(subkeys[2], (), 0, devices - 1)) % devices
    indices = jnp.arange(devices)
    counts = jnp.where(indices == fullest, SEQ_DEV, counts)
    counts = jnp.where(indices == lightest, 1, counts)
    scores = jax.random.randint(subkeys[3], (devices, SEQ_DEV), 0, 1 << 20) * SEQ_DEV + jnp.arange(SEQ_DEV)[None, :]
    ordering = jnp.argsort(jnp.argsort(scores, axis=1), axis=1)
    extents = jax.random.randint(subkeys[4], (devices, SEQ_DEV), SEQ_LEN // 4, SEQ_LEN + 1)
    extents = jnp.where((indices == fullest)[:, None] & (ordering == 0), SEQ_LEN, extents)
    return jnp.where(ordering < counts[:, None], extents, 0).reshape(SEQS).astype(jnp.int32)


def draw_layer_input(key, part):
    key_one, key_two, key_three = jax.random.split(key, 3)
    entries = jnp.clip(jax.random.normal(key_one, (TOKENS, D), jnp.float32), -5.0, 5.0)
    row_scale = jnp.exp(jax.random.uniform(key_two, (TOKENS, 1), jnp.float32, math.log(0.3), math.log(3.0)))
    column_scale = jnp.exp(jax.random.uniform(key_three, (1, D), jnp.float32, math.log(0.5), math.log(2.0)))
    return (entries * row_scale * column_scale).astype(jnp.bfloat16)


def draw_vectors(key, part):
    key_one, key_two = jax.random.split(key, 2)
    gains = jax.random.uniform(key_one, (6, D), jnp.float32, 0.6, 1.4)
    biases = 0.4 * jnp.clip(jax.random.normal(key_two, (6, D), jnp.float32), -4.0, 4.0)
    rows = jnp.arange(6)
    is_gain = (rows % 2 == 0) & (rows < 4)
    return jnp.where(is_gain[:, None], gains, biases)


def moment_pair(key, shape, factor):
    key_one, key_two = jax.random.split(key, 2)
    typical = factor * (0.5 * TOKENS) ** 0.5
    first_moment = jnp.clip(jax.random.normal(key_one, shape, jnp.float32), -5.0, 5.0) * (typical / 9.0)
    root_moment = typical / 19.0 ** 0.5 * jnp.exp(jax.random.uniform(key_two, shape, jnp.float32, 0.5 * math.log(0.3), 0.5 * math.log(3.0)))
    return jnp.stack([first_moment, root_moment])


def draw_projector_moments(key, part):
    return moment_pair(key, (D, 3 * HEADS * HD), 1.0)


def draw_shifts_moments(key, part):
    return moment_pair(key, (HEADS, 3 * HD), (D / max(D // 128, 4)) ** 0.5)


def draw_combiner_moments(key, part):
    return moment_pair(key, (HEADS * HD, D), 0.1)


def draw_expander_moments(key, part):
    return moment_pair(key, (D, FF), 0.25)


def draw_offsets_moments(key, part):
    return moment_pair(key, (HEADS, FF // HEADS), 0.25)


def draw_reducer_moments(key, part):
    return moment_pair(key, (FF, D), 0.5)


def draw_vectors_moments(key, part):
    return moment_pair(key, (6, D), 1.5)


def level_of(rng, shape, shards, smallest, top_value):
    gain, own = 1.0, jax.random.fold_in(rng, 6)
    for dim, blocks in shards:
        heights = jnp.exp(jax.random.uniform(jax.random.fold_in(own, dim), (blocks,), jnp.float32, smallest / len(shards), top_value / len(shards)))
        gain = gain * jnp.repeat(heights, shape[dim] // blocks).reshape([-1 if axis == dim else 1 for axis in range(len(shape))])
    return gain


def noise(rng, extent, width, most, cuts=(), kind=jnp.bfloat16):
    values = width * jax.random.normal(rng, extent, jnp.float32)
    if cuts:
        values = values * level_of(rng, extent, cuts, -0.22, 0.18)
    return jnp.clip(values, -most, most).astype(kind)


def setup_inputs(seed: int = 0) -> dict:
    key_list = jax.random.split(jax.random.key(seed), 18)
    return {
        "layer_input": draw_layer_input(jax.random.fold_in(key_list[17], 71), 0),
        "cotangent": noise(key_list[1], (TOKENS, D), 1.0, 6.0, ((0, 8),)),
        "lengths": draw_lengths(jax.random.fold_in(key_list[17], 71), 0),
        "projector": noise(key_list[3], (D, 3 * HEADS * HD), D ** -0.5, 0.125, ((0, 8), (1, 4)), jnp.float32),
        "projector_moments": draw_projector_moments(jax.random.fold_in(key_list[17], 71), 0),
        "shifts": noise(key_list[5], (HEADS, 3 * HD), 0.5, 3.0, ((0, 4), (1, 8)), jnp.float32),
        "shifts_moments": draw_shifts_moments(jax.random.fold_in(key_list[17], 71), 0),
        "combiner": noise(key_list[7], (HEADS * HD, D), (max(D // 128, 4)) ** -0.5, 1.5, ((0, 4), (1, 8)), jnp.float32),
        "combiner_moments": draw_combiner_moments(jax.random.fold_in(key_list[17], 71), 0),
        "expander": noise(key_list[9], (D, FF), D ** -0.5, 0.125, ((0, 8), (1, 4)), jnp.float32),
        "expander_moments": draw_expander_moments(jax.random.fold_in(key_list[17], 71), 0),
        "offsets": noise(key_list[11], (HEADS, FF // HEADS), 0.5, 3.0, ((0, 4), (1, 8)), jnp.float32),
        "offsets_moments": draw_offsets_moments(jax.random.fold_in(key_list[17], 71), 0),
        "reducer": noise(key_list[13], (FF, D), FF ** -0.5, 0.0625, ((0, 4), (1, 8)), jnp.float32),
        "reducer_moments": draw_reducer_moments(jax.random.fold_in(key_list[17], 71), 0),
        "vectors": draw_vectors(jax.random.fold_in(key_list[17], 71), 0),
        "vectors_moments": draw_vectors_moments(jax.random.fold_in(key_list[17], 71), 0),
    }


layer_eps = 1e-05
adam_eps = 1e-08
beta_one = 0.9
beta_two = 0.95
learn_rate = 0.02
decay_rate = 0.01
rotary_base = 10000.0
highest = lax.Precision.HIGHEST

@jax.custom_vjp
def low(v):
    return lax.optimization_barrier(v.astype(jnp.bfloat16)).astype(jnp.float32)

@jax.custom_vjp
def low_back(v):
    return v

def low_keep(v):
    return (low(v), None)

def low_pass(kept, grad):
    return (grad,)

def back_keep(v):
    return (v, None)

def back_low(kept, grad):
    return (low(grad),)
low.defvjp(low_keep, low_pass)
low_back.defvjp(back_keep, back_low)

def matmul(left, right):
    return jnp.dot(left, right, precision=highest, preferred_element_type=jnp.float32)

def norm_layer(values, scale_row, shift_row):
    average = lax.optimization_barrier(jnp.mean(values, axis=-1, keepdims=True))
    centred = values - average
    variance = lax.optimization_barrier(jnp.mean(centred * centred, axis=-1, keepdims=True))
    return centred * lax.rsqrt(variance + layer_eps) * scale_row + shift_row

def rotary_tables():
    half_rot = ROT // 2
    frequency = jnp.exp(jnp.arange(half_rot, dtype=jnp.float32) * (-2.0 * math.log(rotary_base) / ROT))
    angles = jnp.arange(SEQ_LEN, dtype=jnp.float32)[:, None] * frequency[None, :]
    return (jnp.cos(angles)[:, None, :], jnp.sin(angles)[:, None, :])

def rotate(values, cos_table, sin_table):
    half_rot = ROT // 2
    leading = values[..., :half_rot]
    trailing = values[..., half_rot:ROT]
    return jnp.concatenate([leading * cos_table - trailing * sin_table, trailing * cos_table + leading * sin_table, values[..., ROT:]], axis=-1)

def allowed_mask(length):
    position = jnp.arange(SEQ_LEN)
    return (position[None, :] <= position[:, None]) & (position[None, :] < jnp.maximum(length, 1))

def attend_slot(pieces):
    query_rows, key_rows, value_rows, length = pieces
    scores = low_back(jnp.einsum('qhd,khd->hqk', query_rows, key_rows, precision=highest) * HD ** (-0.5))
    scores = jnp.where(allowed_mask(length)[None], scores, -1e+30)
    weights = jax.nn.softmax(scores, axis=-1)
    return jnp.einsum('hqk,khd->qhd', low(weights), value_rows, precision=highest)

def block_forward(block_lengths, params, block_input):
    projector, shifts, combiner, expander, offsets, reducer, vectors = params
    slot_count = block_lengths.shape[0]
    row_count = slot_count * SEQ_LEN
    cos_table, sin_table = rotary_tables()
    normed_one = low(norm_layer(block_input, vectors[0], vectors[1]))
    packed = low_back(matmul(normed_one, projector) + shifts.reshape(-1))
    packed = packed.reshape(slot_count, SEQ_LEN, HEADS, 3, HD)
    query_rows = low(rotate(packed[:, :, :, 0], cos_table, sin_table))
    key_rows = low(rotate(packed[:, :, :, 1], cos_table, sin_table))
    value_rows = low(packed[:, :, :, 2])
    mixture = lax.map(jax.checkpoint(attend_slot), (query_rows, key_rows, value_rows, block_lengths))
    attended = low(low_back(mixture)).reshape(row_count, HEADS * HD)
    normed_two = low(norm_layer(block_input, vectors[2], vectors[3]))
    hidden = low_back(matmul(normed_two, expander) + offsets.reshape(-1))
    activated = low(jax.nn.gelu(hidden, approximate=False))
    live_rows = (jnp.arange(SEQ_LEN)[None, :] < block_lengths[:, None]).astype(jnp.float32).reshape(row_count, 1)
    return live_rows * (block_input + matmul(attended, combiner) + vectors[4] + matmul(activated, reducer) + vectors[5])

def adamw(master, moments, gradient):
    first_moment = beta_one * moments[0] + (1.0 - beta_one) * gradient
    root_moment = jnp.sqrt(beta_two * moments[1] * moments[1] + (1.0 - beta_two) * gradient * gradient)
    first_hat = first_moment / (1.0 - beta_one ** STEP)
    root_hat = root_moment / math.sqrt(1.0 - beta_two ** STEP)
    update = -learn_rate * (first_hat / (root_hat + adam_eps) + decay_rate * master)
    return (jnp.stack([first_moment, root_moment]), update)

def zero_like(master):
    return jnp.zeros(master.shape, jnp.float32)

def reference(layer_input, cotangent, lengths, projector, projector_moments, shifts, shifts_moments, combiner, combiner_moments, expander, expander_moments, offsets, offsets_moments, reducer, reducer_moments, vectors, vectors_moments):
    masters = (projector, shifts, combiner, expander, offsets, reducer, vectors)
    moments = (projector_moments, shifts_moments, combiner_moments, expander_moments, offsets_moments, reducer_moments, vectors_moments)
    rounded = jax.tree.map(low, masters)
    block_slots = 8
    blocks = SEQS // block_slots
    inputs = layer_input.astype(jnp.float32).reshape(blocks, block_slots * SEQ_LEN, D)
    upstream = cotangent.astype(jnp.float32).reshape(blocks, block_slots * SEQ_LEN, D)
    grouped = lengths.reshape(blocks, block_slots)

    def accumulate(totals, pieces):
        block_input, block_cot, block_len = pieces
        output_rows, pullback = jax.vjp(partial(block_forward, block_len), rounded, block_input)
        param_grads, input_grads = pullback(block_cot)
        return (jax.tree.map(jnp.add, totals, param_grads), (output_rows, input_grads))
    starting = jax.tree.map(zero_like, masters)
    gradients, (outputs, input_grads) = lax.scan(accumulate, starting, (inputs, upstream, grouped))
    layer_output = outputs.reshape(TOKENS, D).astype(jnp.bfloat16)
    input_gradient = input_grads.reshape(TOKENS, D).astype(jnp.bfloat16)
    results = [layer_output, input_gradient]
    for master, moment_set, gradient in zip(masters, moments, gradients):
        states, update = adamw(master, moment_set, gradient)
        results.extend([gradient, states, update])
    return tuple(results)
```

```python
import functools
import math

import jax
import jax.numpy as jnp
from jax import lax
from jax.experimental import pallas as pl
from jax.experimental.pallas import tpu as pltpu
from jax.sharding import PartitionSpec as P

HD = 256
ROT = 64
SEQ_LEN = 512
STEP = 10

layer_eps = 1e-05
adam_eps = 1e-08
beta_one = 0.9
beta_two = 0.95
learn_rate = 0.02
decay_rate = 0.01
rotary_base = 10000.0

TILE = 128
BLOCK = 256
SLOT_TILES = SEQ_LEN // TILE
LEAST = 3
VMEM = 60 * 1024 * 1024
F32 = jnp.float32
BF16 = jnp.bfloat16

GATHER = "sc"
REDUCE = "sc"


def rotary_tables():
    half = ROT // 2
    frequency = jnp.exp(jnp.arange(half, dtype=F32) * (-2.0 * math.log(rotary_base) / ROT))
    angles = jnp.arange(SEQ_LEN, dtype=F32)[:, None] * frequency[None, :]
    cos, sin = jnp.cos(angles), jnp.sin(angles)
    zero = jnp.zeros((SEQ_LEN, half), F32)
    rest = jnp.ones((SEQ_LEN, 128 - ROT), F32)
    pad = jnp.zeros((SEQ_LEN, 128 - ROT), F32)
    return jnp.stack(
        [
            jnp.concatenate([cos, cos, rest], 1),
            jnp.concatenate([-sin, zero, pad], 1),
            jnp.concatenate([zero, sin, pad], 1),
        ]
    )


def turn(values, table_ref, rows, sign):
    head = values[:, :128]
    ahead = pltpu.roll(head, 128 - ROT // 2, 1)
    behind = pltpu.roll(head, ROT // 2, 1)
    swing = ahead * table_ref[1, rows, :] + behind * table_ref[2, rows, :]
    turned = head * table_ref[0, rows, :]
    turned = turned + swing if sign > 0 else turned - swing
    return jnp.concatenate([turned, values[:, 128:]], axis=1)


def slot_tiles(lens_ref, slot):
    return (lens_ref[slot] + (TILE - 1)) // TILE


def live_tiles(lens_ref, slots):
    total = slot_tiles(lens_ref, 0)
    for slot in range(1, slots):
        total = total + slot_tiles(lens_ref, slot)
    return total


def live_blocks(lens_ref, slots):
    return jnp.maximum((live_tiles(lens_ref, slots) + 1) // 2, LEAST)


def source_tile(lens_ref, index, slots):
    start = 0
    source = 0
    for slot in range(slots):
        count = slot_tiles(lens_ref, slot)
        inside = (index >= start) & (index < start + count)
        source = jnp.where(inside, slot * SLOT_TILES + index - start, source)
        start = start + count
    return source


def compact_tile(lens_ref, source, slots):
    slot = source // SLOT_TILES
    within = source % SLOT_TILES
    start = 0
    target = -1
    for other in range(slots):
        count = slot_tiles(lens_ref, other)
        target = jnp.where((slot == other) & (within < count), start + within, target)
        start = start + count
    return target


def norm_parts(values):
    average = jnp.mean(values, axis=-1, keepdims=True)
    centred = values - average
    variance = jnp.mean(centred * centred, axis=-1, keepdims=True)
    return centred, lax.rsqrt(variance + layer_eps)


def norm_rows(lens, layer_input, cotangent, vecs, slots):
    rows, width = layer_input.shape
    tiles = rows // TILE

    def kernel(lens_ref, x_ref, cot_ref, vec_ref, one_ref, two_ref, x_out, up_out):
        i = pl.program_id(0)
        total = live_tiles(lens_ref, slots)
        last = 2 * live_blocks(lens_ref, slots)

        @pl.when(i < total)
        def _():
            source = source_tile(lens_ref, i, slots)
            values = x_ref[...].astype(F32)
            centred, scale = norm_parts(values)
            hat = centred * scale
            one_ref[...] = (hat * vec_ref[0:1, :] + vec_ref[1:2, :]).astype(BF16)
            two_ref[...] = (hat * vec_ref[2:3, :] + vec_ref[3:4, :]).astype(BF16)
            x_out[...] = x_ref[...]
            length = lens_ref[source // SLOT_TILES]
            place = (source % SLOT_TILES) * TILE + lax.broadcasted_iota(jnp.int32, (TILE, 1), 0)
            up_out[...] = jnp.where(place < length, cot_ref[...].astype(F32), 0.0).astype(BF16)

        @pl.when((i >= total) & (i < last))
        def _():
            for ref in (one_ref, two_ref, x_out, up_out):
                ref[...] = jnp.zeros_like(ref)

    def reads(i, lens_ref):
        total = jnp.maximum(live_tiles(lens_ref, slots), 1)
        return (source_tile(lens_ref, jnp.minimum(i, total - 1), slots), 0)

    def writes(i, lens_ref):
        return (jnp.minimum(i, 2 * live_blocks(lens_ref, slots) - 1), 0)

    shape = jax.ShapeDtypeStruct((rows, width), BF16)
    return pl.pallas_call(
        kernel,
        out_shape=(shape,) * 4,
        grid_spec=pltpu.PrefetchScalarGridSpec(
            num_scalar_prefetch=1,
            grid=(tiles,),
            in_specs=[
                pl.BlockSpec((TILE, width), reads),
                pl.BlockSpec((TILE, width), reads),
                pl.BlockSpec(vecs.shape, lambda i, lens_ref: (0, 0)),
            ],
            out_specs=[pl.BlockSpec((TILE, width), writes)] * 4,
        ),
        compiler_params=pltpu.CompilerParams(vmem_limit_bytes=VMEM),
        cost_estimate=pl.CostEstimate(
            flops=rows * width * 8, bytes_accessed=rows * width * 12, transcendentals=0
        ),
        name="norm_rows",
    )(lens, layer_input, cotangent, vecs)


class Gathered:
    def __init__(self, pieces, shard):
        self.pieces = [piece for piece, _, _ in pieces]
        self.places = [(mask, extra) for _, mask, extra in pieces]
        self.shard = shard
        self.width = self.pieces[0].shape[1]

    def copies(self, refs, target, sems):
        if self.places[0][0] is not None:
            me = lax.axis_index("dp")
        out = []
        for index, (ref, (mask, extra)) in enumerate(zip(refs, self.places)):
            count = ref.shape[0]
            start = 0 if mask is None else (me ^ mask) * self.shard + extra
            start = start if mask is None else pl.multiple_of(start, count)
            out.append(
                pltpu.make_async_copy(ref, target.at[pl.ds(start, count), :], sems.at[index])
            )
        return out


def any_specs(count):
    return [pl.BlockSpec(memory_space=pl.ANY)] * count


def project_rows(lens, normed, upstream, weights, shift_row, table, slots, qkv_width):
    rows, width = normed.shape
    att_width = weights.width - qkv_width
    blocks = rows // BLOCK
    count = len(weights.pieces)

    def kernel(lens_ref, n_ref, up_ref, shift_ref, table_ref, *rest):
        refs, (qkv_ref, back_ref, held, sems) = rest[:count], rest[count:]
        i = pl.program_id(0)

        @pl.when(i == 0)
        def _():
            copies = weights.copies(refs, held, sems)
            for copy in copies:
                copy.start()
            for copy in copies:
                copy.wait()

        @pl.when(i < live_blocks(lens_ref, slots))
        def _():
            for piece in range(qkv_width // HD):
                cols = slice(piece * HD, (piece + 1) * HD)
                part = jnp.dot(n_ref[...], held[:, cols], preferred_element_type=F32)
                part = part + shift_ref[0:1, cols]
                if piece % 3 == 2:
                    qkv_ref[:, cols] = part.astype(BF16)
                    continue
                for half in range(BLOCK // TILE):
                    tile = slice(half * TILE, (half + 1) * TILE)
                    source = source_tile(lens_ref, i * (BLOCK // TILE) + half, slots)
                    place = pl.multiple_of((source % SLOT_TILES) * TILE, TILE)
                    qkv_ref[tile, cols] = turn(
                        part[tile], table_ref, pl.ds(place, TILE), 1
                    ).astype(BF16)
            back_ref[...] = jnp.dot(
                up_ref[...], held[:, qkv_width:], preferred_element_type=F32
            ).astype(BF16)

    def block(i, lens_ref):
        return (jnp.minimum(i, live_blocks(lens_ref, slots) - 1), 0)

    whole2 = lambda i, lens_ref: (0, 0)
    return pl.pallas_call(
        kernel,
        out_shape=(
            jax.ShapeDtypeStruct((rows, qkv_width), BF16),
            jax.ShapeDtypeStruct((rows, att_width), BF16),
        ),
        grid_spec=pltpu.PrefetchScalarGridSpec(
            num_scalar_prefetch=1,
            grid=(blocks,),
            in_specs=[
                pl.BlockSpec((BLOCK, width), block),
                pl.BlockSpec((BLOCK, width), block),
                pl.BlockSpec(shift_row.shape, whole2),
                pl.BlockSpec(table.shape, lambda i, lens_ref: (0, 0, 0)),
            ]
            + any_specs(count),
            out_specs=[
                pl.BlockSpec((BLOCK, qkv_width), block),
                pl.BlockSpec((BLOCK, att_width), block),
            ],
            scratch_shapes=[
                pltpu.VMEM((width, weights.width), BF16),
                pltpu.SemaphoreType.DMA((count,)),
            ],
        ),
        compiler_params=pltpu.CompilerParams(vmem_limit_bytes=VMEM),
        cost_estimate=pl.CostEstimate(
            flops=2 * rows * width * weights.width,
            bytes_accessed=rows * width * 8,
            transcendentals=0,
        ),
        name="project_rows",
    )(lens, normed, upstream, shift_row, table, *weights.pieces)


def attend(lens, qkv, back, table, slots):
    rows, qkv_width = qkv.shape
    heads = qkv_width // (3 * HD)
    scale = HD ** (-0.5)

    def kernel(lens_ref, qkv_ref, back_ref, table_ref, att_ref, grad_ref, sum_ref, dk_acc, dv_acc):
        slot = pl.program_id(1)
        start = 0
        count = 0
        length = 0
        total = 0
        for other in range(slots):
            own = slot_tiles(lens_ref, other)
            start = jnp.where(other < slot, start + own, start)
            count = jnp.where(other == slot, own, count)
            length = jnp.where(other == slot, lens_ref[other], length)
            total = total + own
        limit = jnp.maximum(length, 1)

        @pl.when(slot == 0)
        def _():
            sum_ref[...] = jnp.zeros_like(sum_ref)
            for index in range(2 * LEAST + 6):
                if index * TILE < rows:
                    dead = (index >= total) & (index < 2 * live_blocks(lens_ref, slots))

                    @pl.when(dead)
                    def _(index=index):
                        tile = slice(index * TILE, (index + 1) * TILE)
                        att_ref[tile, :] = jnp.zeros((TILE, HD), BF16)
                        grad_ref[tile, :] = jnp.zeros((TILE, 3 * HD), BF16)

        base = start * TILE
        dot_nt = lambda a, b: lax.dot_general(
            a, b, (((1,), (1,)), ((), ())), preferred_element_type=F32
        )
        dot_tn = lambda a, b: lax.dot_general(
            a, b, (((0,), (0,)), ((), ())), preferred_element_type=F32
        )

        def keep_sum(value, cols):
            sum_ref[0:1, cols] += jnp.sum(value.astype(F32), axis=0, keepdims=True)

        for i in range(SLOT_TILES):

            @pl.when(count > i)
            def _(i=i):
                span = (i + 1) * TILE
                mine = pl.ds(pl.multiple_of(base + i * TILE, TILE), TILE)
                seen = pl.ds(pl.multiple_of(base, TILE), span)
                query = qkv_ref[mine, 0:HD]
                keys = qkv_ref[seen, HD : 2 * HD]
                values = qkv_ref[seen, 2 * HD : 3 * HD]
                push = back_ref[mine, :]
                place = i * TILE + lax.broadcasted_iota(jnp.int32, (TILE, span), 0)
                column = lax.broadcasted_iota(jnp.int32, (TILE, span), 1)
                allowed = (column <= place) & (column < limit)
                scores = jnp.where(allowed, dot_nt(query, keys) * scale, -1e30)
                powers = jnp.exp(scores - jnp.max(scores, axis=-1, keepdims=True))
                weights = powers / jnp.sum(powers, axis=-1, keepdims=True)
                low = weights.astype(BF16)
                att_ref[mine, :] = jnp.dot(low, values, preferred_element_type=F32).astype(BF16)
                pushed = dot_nt(push, values)
                inner = jnp.sum(weights * pushed, axis=-1, keepdims=True)
                dscores = (weights * (pushed - inner)).astype(BF16)
                dquery = jnp.dot(dscores, keys, preferred_element_type=F32) * scale
                dquery = turn(dquery, table_ref, slice(i * TILE, span), -1).astype(BF16)
                grad_ref[mine, 0:HD] = dquery
                keep_sum(dquery, slice(0, HD))
                dkeys = dot_tn(dscores, query)
                dvalues = dot_tn(low, push)
                if i > 0:
                    dk_acc[0 : i * TILE, :] += dkeys[0 : i * TILE]
                    dv_acc[0 : i * TILE, :] += dvalues[0 : i * TILE]
                dk_acc[i * TILE : span, :] = dkeys[i * TILE : span]
                dv_acc[i * TILE : span, :] = dvalues[i * TILE : span]

        for i in range(SLOT_TILES):

            @pl.when(count > i)
            def _(i=i):
                tile = slice(i * TILE, (i + 1) * TILE)
                mine = pl.ds(pl.multiple_of(base + i * TILE, TILE), TILE)
                dkeys = turn(dk_acc[tile, :] * scale, table_ref, tile, -1).astype(BF16)
                dvalues = dv_acc[tile, :].astype(BF16)
                grad_ref[mine, HD : 2 * HD] = dkeys
                grad_ref[mine, 2 * HD : 3 * HD] = dvalues
                keep_sum(dkeys, slice(HD, 2 * HD))
                keep_sum(dvalues, slice(2 * HD, 3 * HD))

    by_head = lambda h, s, lens_ref: (0, h)
    return pl.pallas_call(
        kernel,
        out_shape=(
            jax.ShapeDtypeStruct((rows, heads * HD), BF16),
            jax.ShapeDtypeStruct((rows, qkv_width), BF16),
            jax.ShapeDtypeStruct((8, qkv_width), F32),
        ),
        grid_spec=pltpu.PrefetchScalarGridSpec(
            num_scalar_prefetch=1,
            grid=(heads, slots),
            in_specs=[
                pl.BlockSpec((rows, 3 * HD), by_head),
                pl.BlockSpec((rows, HD), by_head),
                pl.BlockSpec(table.shape, lambda h, s, lens_ref: (0, 0, 0)),
            ],
            out_specs=[
                pl.BlockSpec((rows, HD), by_head),
                pl.BlockSpec((rows, 3 * HD), by_head),
                pl.BlockSpec((8, 3 * HD), by_head),
            ],
            scratch_shapes=[pltpu.VMEM((SEQ_LEN, HD), F32), pltpu.VMEM((SEQ_LEN, HD), F32)],
        ),
        compiler_params=pltpu.CompilerParams(vmem_limit_bytes=VMEM),
        cost_estimate=pl.CostEstimate(
            flops=14 * heads * slots * SEQ_LEN * SEQ_LEN * HD,
            bytes_accessed=rows * qkv_width * 6,
            transcendentals=heads * slots * SEQ_LEN * SEQ_LEN,
        ),
        name="attend",
    )(lens, qkv, back, table)


def middle(lens, first, span, tensors, vecs, offset_row, entry, expand, shrink, carried, slots):
    normed, upstream, attended, dpacked, inputs = tensors
    rows, width = normed.shape
    hidden_width = expand.width
    qkv_width = dpacked.shape[1]
    att_width = attended.shape[1]
    counts = [len(entry.pieces), len(expand.pieces), len(shrink.pieces)]
    total = sum(counts)
    hold = 2 if carried is not None else 0
    chunk = 512
    nt = (((1,), (1,)), ((), ()))

    def kernel(lens_ref, n_ref, up_ref, att_ref, dp_ref, x_ref, vec_ref, off_ref, *rest):
        refs = rest[:total]
        rest = rest[total + hold :]
        act_ref, dh_ref, both_ref, sum_ref = rest[:4]
        held_e, held_x, held_s, done, dtwo, sems_e, sems_x, sems_s = rest[4:]
        i = pl.program_id(0)

        def fetch():
            a, b = counts[0], counts[0] + counts[1]
            return (
                expand.copies(refs[a:b], held_x, sems_x),
                shrink.copies(refs[b:], held_s, sems_s),
                entry.copies(refs[:a], held_e, sems_e),
            )

        @pl.when(i == 0)
        def _():
            sum_ref[...] = jnp.zeros_like(sum_ref)
            for group in fetch():
                for copy in group:
                    copy.start()
            for copy in fetch()[0]:
                copy.wait()
            for copy in fetch()[1]:
                copy.wait()
            for copy in fetch()[2]:
                copy.wait()

        @pl.when(first + i < live_blocks(lens_ref, slots))
        def _():
            for start in range(0, hidden_width, chunk):
                cols = slice(start, start + chunk)
                hidden = jnp.dot(n_ref[...], held_x[:, cols], preferred_element_type=F32)
                hidden = hidden + off_ref[0:1, cols]
                dact = jnp.dot(up_ref[...], held_s[:, cols], preferred_element_type=F32)
                below = 0.5 + 0.5 * lax.erf(hidden * (0.5**0.5))
                slope = below + hidden * (
                    jnp.exp(-0.5 * hidden * hidden) * ((2.0 * math.pi) ** -0.5)
                )
                act_ref[:, cols] = (hidden * below).astype(BF16)
                dhidden = (dact * slope).astype(BF16)
                dh_ref[:, cols] = dhidden
                sum_ref[5:6, cols] += jnp.sum(dhidden.astype(F32), axis=0, keepdims=True)
            values = x_ref[...].astype(F32)
            centred, scale = norm_parts(values)
            hat = centred * scale
            mean_e = jnp.zeros((BLOCK, 1), F32)
            mean_eh = jnp.zeros((BLOCK, 1), F32)
            for start in range(0, width, chunk):
                cols = slice(start, start + chunk)
                part = lax.dot_general(
                    att_ref[...], held_e[cols, qkv_width:], nt, preferred_element_type=F32
                ) + lax.dot_general(
                    act_ref[...], held_s[cols, :], nt, preferred_element_type=F32
                )
                both_ref[0, :, cols] = part.astype(BF16)
            for start in range(0, width, chunk):
                cols = slice(start, start + chunk)
                two = lax.dot_general(
                    dh_ref[...], held_x[cols, :], nt, preferred_element_type=F32
                )
                one = lax.dot_general(
                    dp_ref[...], held_e[cols, :qkv_width], nt, preferred_element_type=F32
                )
                part = hat[:, cols]
                sum_ref[0:1, cols] += jnp.sum(one * part, axis=0, keepdims=True)
                sum_ref[1:2, cols] += jnp.sum(one, axis=0, keepdims=True)
                sum_ref[2:3, cols] += jnp.sum(two * part, axis=0, keepdims=True)
                sum_ref[3:4, cols] += jnp.sum(two, axis=0, keepdims=True)
                sum_ref[4:5, cols] += jnp.sum(up_ref[:, cols].astype(F32), axis=0, keepdims=True)
                err = one * vec_ref[0:1, cols] + two * vec_ref[2:3, cols]
                done[:, cols] = err
                mean_e = mean_e + jnp.sum(err, axis=-1, keepdims=True)
                mean_eh = mean_eh + jnp.sum(err * part, axis=-1, keepdims=True)
            mean_e = mean_e * (1.0 / width)
            mean_eh = mean_eh * (1.0 / width)
            for start in range(0, width, chunk):
                cols = slice(start, start + chunk)
                both_ref[1, :, cols] = (
                    scale * (done[:, cols] - mean_e - hat[:, cols] * mean_eh)
                ).astype(BF16)

    def block(i, lens_ref):
        return (jnp.minimum(first + i, live_blocks(lens_ref, slots) - 1), 0)

    def local(i, lens_ref):
        top = jnp.maximum(live_blocks(lens_ref, slots) - 1 - first, 0)
        return (0, jnp.minimum(i, top), 0)

    def kept(i, lens_ref):
        top = jnp.maximum(live_blocks(lens_ref, slots) - 1, first)
        return (jnp.minimum(first + i, top), 0)

    whole2 = lambda i, lens_ref: (0, 0)
    sum_width = max(width, hidden_width)
    hidden_shape = jax.ShapeDtypeStruct((rows, hidden_width), BF16)
    args = [lens, normed, upstream, attended, dpacked, inputs, vecs, offset_row]
    args += entry.pieces + expand.pieces + shrink.pieces
    aliases = {}
    if carried is not None:
        aliases = {len(args): 0, len(args) + 1: 1}
        args += list(carried)
    return pl.pallas_call(
        kernel,
        out_shape=(
            hidden_shape,
            hidden_shape,
            jax.ShapeDtypeStruct((2, span * BLOCK, width), BF16),
            jax.ShapeDtypeStruct((8, sum_width), F32),
        ),
        grid_spec=pltpu.PrefetchScalarGridSpec(
            num_scalar_prefetch=1,
            grid=(span,),
            in_specs=[
                pl.BlockSpec((BLOCK, width), block),
                pl.BlockSpec((BLOCK, width), block),
                pl.BlockSpec((BLOCK, att_width), block),
                pl.BlockSpec((BLOCK, qkv_width), block),
                pl.BlockSpec((BLOCK, width), block),
                pl.BlockSpec(vecs.shape, whole2),
                pl.BlockSpec(offset_row.shape, whole2),
            ]
            + any_specs(total + hold),
            out_specs=[
                pl.BlockSpec((BLOCK, hidden_width), kept),
                pl.BlockSpec((BLOCK, hidden_width), kept),
                pl.BlockSpec((2, BLOCK, width), local),
                pl.BlockSpec((8, sum_width), whole2),
            ],
            scratch_shapes=[
                pltpu.VMEM((width, entry.width), BF16),
                pltpu.VMEM((width, expand.width), BF16),
                pltpu.VMEM((width, shrink.width), BF16),
                pltpu.VMEM((BLOCK, width), F32),
                pltpu.VMEM((8, 128), F32),
            ]
            + [pltpu.SemaphoreType.DMA((count,)) for count in (counts[1], counts[2], counts[0])][:0]
            + [
                pltpu.SemaphoreType.DMA((counts[0],)),
                pltpu.SemaphoreType.DMA((counts[1],)),
                pltpu.SemaphoreType.DMA((counts[2],)),
            ],
        ),
        input_output_aliases=aliases,
        compiler_params=pltpu.CompilerParams(vmem_limit_bytes=VMEM),
        cost_estimate=pl.CostEstimate(
            flops=2 * span * BLOCK * width * (4 * hidden_width + qkv_width + att_width),
            bytes_accessed=3 * width * hidden_width * 2 + span * BLOCK * width * 16,
            transcendentals=2 * span * BLOCK * hidden_width,
        ),
        name="middle",
    )(*args)


def gradient(lens, pairs, slots, shard, split):
    rows, width = pairs[0][0].shape
    blocks = width // shard
    sizes = [right.shape[1] for _, right in pairs]
    total = sum(sizes)
    half = blocks // 2
    most = rows // BLOCK

    def kernel(lens_ref, *rest):
        lefts = rest[: len(pairs)]
        rights = rest[len(pairs) : 2 * len(pairs)]
        outs = rest[2 * len(pairs) :]
        j = pl.program_id(0)
        live = live_blocks(lens_ref, slots)

        def emit(ref, depth):
            start = 0
            for left, right, size in zip(lefts, rights, sizes):
                ref[0, :, start : start + size] = lax.dot_general(
                    left[: depth * BLOCK, :],
                    right[: depth * BLOCK, :],
                    (((0,), (0,)), ((), ())),
                    preferred_element_type=F32,
                ).astype(BF16)
                start += size

        for depth in range(LEAST, most + 1):
            match = live == depth
            if split:
                for which, ref in enumerate(outs):
                    here = (j >= half) if which else (j < half)

                    @pl.when(match & here)
                    def _(ref=ref, depth=depth):
                        emit(ref, depth)

            else:

                @pl.when(match)
                def _(depth=depth):
                    emit(outs[0], depth)

    def left_block(j, lens_ref):
        if not split:
            return (0, j)
        mask = jnp.where(j < half, 2 * j + 1, 2 * (j - half))
        return (0, lens_ref[slots] ^ mask)

    whole2 = lambda j, lens_ref: (0, 0)
    if split:
        out_shape = [jax.ShapeDtypeStruct((half, shard, total), BF16)] * 2
        out_specs = [
            pl.BlockSpec((1, shard, total), lambda j, lens_ref: (jnp.minimum(j, half - 1), 0, 0)),
            pl.BlockSpec((1, shard, total), lambda j, lens_ref: (jnp.maximum(j - half, 0), 0, 0)),
        ]
    else:
        out_shape = [jax.ShapeDtypeStruct((blocks, shard, total), BF16)]
        out_specs = [pl.BlockSpec((1, shard, total), lambda j, lens_ref: (j, 0, 0))]
    return pl.pallas_call(
        kernel,
        out_shape=out_shape,
        grid_spec=pltpu.PrefetchScalarGridSpec(
            num_scalar_prefetch=1,
            grid=(blocks,),
            in_specs=[pl.BlockSpec((rows, shard), left_block) for _ in pairs]
            + [pl.BlockSpec(right.shape, whole2) for _, right in pairs],
            out_specs=out_specs,
        ),
        compiler_params=pltpu.CompilerParams(vmem_limit_bytes=VMEM),
        cost_estimate=pl.CostEstimate(
            flops=2 * rows * width * total,
            bytes_accessed=rows * (width + total) * 2 + width * total * 2,
            transcendentals=0,
        ),
        name="gradient",
    )(lens, *[left for left, _ in pairs], *[right for _, right in pairs])


def finish_rows(lens, layer_input, cotangent, summed, bias_row, slots):
    rows = layer_input.shape[0]
    width = summed.shape[2]
    tiles = rows // TILE

    def kernel(lens_ref, x_ref, cot_ref, sum_ref, bias_ref, out_ref, grad_ref):
        i = pl.program_id(0)
        target = compact_tile(lens_ref, i, slots)

        @pl.when(target >= 0)
        def _():
            length = lens_ref[i // SLOT_TILES]
            place = (i % SLOT_TILES) * TILE + lax.broadcasted_iota(jnp.int32, (TILE, 1), 0)
            live = place < length
            total = x_ref[...].astype(F32) + sum_ref[0].astype(F32) + bias_ref[0:1, :]
            out_ref[...] = jnp.where(live, total, 0.0).astype(BF16)
            grad = cot_ref[...].astype(F32) + sum_ref[1].astype(F32)
            grad_ref[...] = jnp.where(live, grad, 0.0).astype(BF16)

        @pl.when(target < 0)
        def _():
            out_ref[...] = jnp.zeros_like(out_ref)
            grad_ref[...] = jnp.zeros_like(grad_ref)

    def own(i, lens_ref):
        return (i, lens_ref[slots + 1])

    def packed(i, lens_ref):
        return (0, jnp.maximum(compact_tile(lens_ref, i, slots), 0), 0)

    shape = jax.ShapeDtypeStruct((rows, width), BF16)
    return pl.pallas_call(
        kernel,
        out_shape=(shape, shape),
        grid_spec=pltpu.PrefetchScalarGridSpec(
            num_scalar_prefetch=1,
            grid=(tiles,),
            in_specs=[
                pl.BlockSpec((TILE, width), own),
                pl.BlockSpec((TILE, width), own),
                pl.BlockSpec((2, TILE, width), packed),
                pl.BlockSpec(bias_row.shape, lambda i, lens_ref: (0, 0)),
            ],
            out_specs=[pl.BlockSpec((TILE, width), lambda i, lens_ref: (i, 0))] * 2,
        ),
        cost_estimate=pl.CostEstimate(
            flops=rows * width * 4, bytes_accessed=rows * width * 12, transcendentals=0
        ),
        name="finish_rows",
    )(lens, layer_input, cotangent, summed, bias_row)


def adamw(master, moments, gradient):
    first_moment = beta_one * moments[0] + (1.0 - beta_one) * gradient
    root_moment = jnp.sqrt(
        beta_two * moments[1] * moments[1] + (1.0 - beta_two) * gradient * gradient
    )
    first_hat = first_moment / (1.0 - beta_one**STEP)
    root_hat = root_moment / math.sqrt(1.0 - beta_two**STEP)
    update = -learn_rate * (first_hat / (root_hat + adam_eps) + decay_rate * master)
    return (jnp.stack([first_moment, root_moment]), update)


def swap(values, mask, size):
    return lax.ppermute(values, "dp", [(i, i ^ mask) for i in range(size)])


def after(values, *others):
    return lax.optimization_barrier((values, *others))[0]


def gather_weight(own):
    size = lax.axis_size("dp")
    return Gathered([(lax.all_gather(own, "dp", axis=0, tiled=True), None, 0)], own.shape[0])


def reduce_pieces(pieces):
    return lax.psum_scatter(pieces[0], "dp", scatter_dimension=0, tiled=True)[0].astype(F32)


def on_device(
    layer_input,
    cotangent,
    lengths,
    projector,
    projector_moments,
    shifts,
    shifts_moments,
    combiner,
    combiner_moments,
    expander,
    expander_moments,
    offsets,
    offsets_moments,
    reducer,
    reducer_moments,
    vectors,
    vectors_moments,
):
    dp, tensor = lax.axis_size("dp"), lax.axis_size("tensor")
    rank, lane = lax.axis_index("dp"), lax.axis_index("tensor")
    slots = lengths.shape[0]
    rows, width = layer_input.shape
    shard = projector.shape[0]
    qkv_width = projector.shape[1]
    att_width = combiner.shape[0]
    hidden_width = expander.shape[1]
    lens = jnp.concatenate(
        [lengths, jnp.stack([rank, lane]).astype(jnp.int32), jnp.zeros((3,), jnp.int32)]
    )
    table = rotary_tables()

    entry_own = jnp.concatenate([projector.astype(BF16), combiner.astype(BF16).T], axis=1)
    expand_own = expander.astype(BF16)
    shrink_own = reducer.astype(BF16).T

    sizes = [vectors.size, shifts.size, offsets.size]
    small = jnp.concatenate([vectors.reshape(-1), shifts.reshape(-1), offsets.reshape(-1)])
    small = jnp.pad(small, (0, -small.size % 1024)).astype(BF16).reshape(1, -1)
    small = lax.all_gather(small, ("dp", "tensor"), axis=0, tiled=True).astype(F32)
    full_vectors = (
        small[:, : sizes[0]].reshape(dp * tensor, *vectors.shape).transpose(1, 0, 2).reshape(6, -1)
    )
    biases = lax.dynamic_index_in_dim(
        small.reshape(dp, tensor, -1), lane, axis=1, keepdims=False
    )
    shift_row = (
        biases[:, sizes[0] : sizes[0] + sizes[1]]
        .reshape(dp, *shifts.shape)
        .transpose(1, 0, 2)
        .reshape(1, -1)
    )
    offset_row = (
        biases[:, sizes[0] + sizes[1] : sum(sizes)]
        .reshape(dp, *offsets.shape)
        .transpose(1, 0, 2)
        .reshape(1, -1)
    )
    vecs = jnp.pad(full_vectors, ((0, 2), (0, 0)))

    entry = gather_weight(entry_own)
    expand = gather_weight(expand_own)
    shrink = gather_weight(shrink_own)

    normed_one, normed_two, inputs, upstream = norm_rows(lens, layer_input, cotangent, vecs, slots)
    qkv, back = project_rows(
        lens, normed_one, upstream, entry, shift_row, table, slots, qkv_width
    )
    attended, dpacked, shift_sum = attend(lens, qkv, back, table, slots)
    split = False
    entry_parts = gradient(lens, [(normed_one, dpacked), (upstream, attended)], slots, shard, split)

    blocks = rows // BLOCK
    tensors = (normed_two, upstream, attended, dpacked, inputs)
    carried = None
    sums = 0.0
    reduced = []
    first = 0
    for span in (1, 2, blocks - 3):
        act, dhid, both, part = middle(
            lens, first, span, tensors, vecs, offset_row, entry, expand, shrink, carried, slots
        )
        carried = (act, dhid)
        sums = sums + part
        first += span
        reduced.append(
            lax.psum_scatter(both, "tensor", scatter_dimension=2, tiled=True)
        )
    shrink_parts = gradient(lens, [(upstream, act)], slots, shard, split)
    expand_parts = gradient(lens, [(normed_two, dhid)], slots, shard, split)

    entry_share = reduce_pieces(entry_parts)
    shrink_share = reduce_pieces(shrink_parts)
    expand_share = reduce_pieces(expand_parts)
    projector_grad = entry_share[:, :qkv_width]
    combiner_grad = entry_share[:, qkv_width:].T
    reducer_grad = shrink_share.T
    expander_grad = expand_share

    shift_part = shift_sum[0].reshape(shifts.shape[0], dp, -1).transpose(1, 0, 2).reshape(dp, -1)
    offset_part = (
        sums[5, :hidden_width].reshape(offsets.shape[0], dp, -1).transpose(1, 0, 2).reshape(dp, -1)
    )
    vector_part = sums[:5, :width].reshape(5, dp, -1).transpose(1, 0, 2).reshape(dp, -1)
    packed = jnp.concatenate([vector_part, shift_part, offset_part], axis=1)
    used = packed.shape[1]
    packed = jnp.pad(packed, ((0, 0), (0, -used % 1024)))
    packed = lax.psum_scatter(packed, "dp", scatter_dimension=0, tiled=True)[0]
    vector_part = packed[: vector_part.shape[1]].reshape(5, tensor, -1)
    begin = vector_part.size
    shifts_grad = packed[begin : begin + shifts.size].reshape(shifts.shape)
    offsets_grad = packed[begin + shifts.size : used].reshape(offsets.shape)
    norm_grad = lax.psum_scatter(
        vector_part[:4].transpose(1, 0, 2).reshape(tensor, -1),
        "tensor",
        scatter_dimension=0,
        tiled=True,
    ).reshape(4, -1)
    bias_grad = lax.dynamic_index_in_dim(vector_part[4], lane, axis=0, keepdims=True)
    vectors_grad = jnp.concatenate([norm_grad, bias_grad, bias_grad], axis=0)

    own_width = reduced[0].shape[2]
    own_bias = lax.dynamic_slice_in_dim(
        full_vectors[4] + full_vectors[5], lane * own_width, own_width, 0
    ).reshape(1, -1)
    layer_output, input_gradient = finish_rows(
        lens, layer_input, cotangent, jnp.concatenate(reduced, axis=1), own_bias, slots
    )

    results = [layer_output, input_gradient]
    for master, moments, grad in (
        (projector, projector_moments, projector_grad),
        (shifts, shifts_moments, shifts_grad),
        (combiner, combiner_moments, combiner_grad),
        (expander, expander_moments, expander_grad),
        (offsets, offsets_moments, offsets_grad),
        (reducer, reducer_moments, reducer_grad),
        (vectors, vectors_moments, vectors_grad),
    ):
        states, update = adamw(master, moments, grad)
        results += [grad, states, update]
    return tuple(results)


def solution(mesh):
    rows = P("dp", "tensor")
    cols = P("tensor", "dp")
    deep_rows = P(None, "dp", "tensor")
    deep_cols = P(None, "tensor", "dp")
    both = P(None, ("dp", "tensor"))
    deep_both = P(None, None, ("dp", "tensor"))
    placed = (P("dp", None), P("dp", None), P("dp"))
    results = (rows, rows)
    for plain, deep in (
        (rows, deep_rows),
        (cols, deep_cols),
        (cols, deep_cols),
        (rows, deep_rows),
        (cols, deep_cols),
        (cols, deep_cols),
        (both, deep_both),
    ):
        placed += (plain, deep)
        results += (plain, deep, plain)
    return jax.shard_map(
        on_device, mesh=mesh, in_specs=placed, out_specs=results, check_vma=False
    )
```

```python
import functools
import math

import jax
import jax.numpy as jnp
from jax import lax
from jax.experimental import pallas as pl
from jax.experimental.pallas import tpu as pltpu
from jax.sharding import PartitionSpec as P

HD = 256
ROT = 64
SEQ_LEN = 512
STEP = 10

layer_eps = 1e-05
adam_eps = 1e-08
beta_one = 0.9
beta_two = 0.95
learn_rate = 0.02
decay_rate = 0.01
rotary_base = 10000.0

TILE = 128
BLOCK = 256
SLOT_TILES = SEQ_LEN // TILE
LEAST = 3
VMEM = 60 * 1024 * 1024
F32 = jnp.float32
BF16 = jnp.bfloat16

MESH = pl.DeviceIdType.MESH


def rotary_tables():
    half = ROT // 2
    frequency = jnp.exp(jnp.arange(half, dtype=F32) * (-2.0 * math.log(rotary_base) / ROT))
    angles = jnp.arange(SEQ_LEN, dtype=F32)[:, None] * frequency[None, :]
    cos, sin = jnp.cos(angles), jnp.sin(angles)
    zero = jnp.zeros((SEQ_LEN, half), F32)
    rest = jnp.ones((SEQ_LEN, 128 - ROT), F32)
    pad = jnp.zeros((SEQ_LEN, 128 - ROT), F32)
    return jnp.stack(
        [
            jnp.concatenate([cos, cos, rest], 1),
            jnp.concatenate([-sin, zero, pad], 1),
            jnp.concatenate([zero, sin, pad], 1),
        ]
    )


def turn(values, table_ref, rows, sign):
    head = values[:, :128]
    ahead = pltpu.roll(head, 128 - ROT // 2, 1)
    behind = pltpu.roll(head, ROT // 2, 1)
    swing = ahead * table_ref[1, rows, :] + behind * table_ref[2, rows, :]
    turned = head * table_ref[0, rows, :]
    turned = turned + swing if sign > 0 else turned - swing
    return jnp.concatenate([turned, values[:, 128:]], axis=1)


def slot_tiles(lens_ref, slot):
    return (lens_ref[slot] + (TILE - 1)) // TILE


def live_tiles(lens_ref, slots):
    total = slot_tiles(lens_ref, 0)
    for slot in range(1, slots):
        total = total + slot_tiles(lens_ref, slot)
    return total


def live_blocks(lens_ref, slots):
    return jnp.maximum((live_tiles(lens_ref, slots) + 1) // 2, LEAST)


def source_tile(lens_ref, index, slots):
    start = 0
    source = 0
    for slot in range(slots):
        count = slot_tiles(lens_ref, slot)
        inside = (index >= start) & (index < start + count)
        source = jnp.where(inside, slot * SLOT_TILES + index - start, source)
        start = start + count
    return source


def compact_tile(lens_ref, source, slots):
    slot = source // SLOT_TILES
    within = source % SLOT_TILES
    start = 0
    target = -1
    for other in range(slots):
        count = slot_tiles(lens_ref, other)
        target = jnp.where((slot == other) & (within < count), start + within, target)
        start = start + count
    return target


def norm_parts(values):
    average = jnp.mean(values, axis=-1, keepdims=True)
    centred = values - average
    variance = jnp.mean(centred * centred, axis=-1, keepdims=True)
    return centred, lax.rsqrt(variance + layer_eps)


def norm_rows(lens, layer_input, cotangent, vecs, slots):
    rows, width = layer_input.shape
    tiles = rows // TILE

    def kernel(lens_ref, x_ref, cot_ref, vec_ref, one_ref, two_ref, x_out, up_out):
        i = pl.program_id(0)
        total = live_tiles(lens_ref, slots)
        last = 2 * live_blocks(lens_ref, slots)

        @pl.when(i < total)
        def _():
            source = source_tile(lens_ref, i, slots)
            values = x_ref[...].astype(F32)
            centred, scale = norm_parts(values)
            hat = centred * scale
            one_ref[...] = (hat * vec_ref[0:1, :] + vec_ref[1:2, :]).astype(BF16)
            two_ref[...] = (hat * vec_ref[2:3, :] + vec_ref[3:4, :]).astype(BF16)
            x_out[...] = x_ref[...]
            length = lens_ref[source // SLOT_TILES]
            place = (source % SLOT_TILES) * TILE + lax.broadcasted_iota(jnp.int32, (TILE, 1), 0)
            up_out[...] = jnp.where(place < length, cot_ref[...].astype(F32), 0.0).astype(BF16)

        @pl.when((i >= total) & (i < last))
        def _():
            for ref in (one_ref, two_ref, x_out, up_out):
                ref[...] = jnp.zeros_like(ref)

    def reads(i, lens_ref):
        total = jnp.maximum(live_tiles(lens_ref, slots), 1)
        return (source_tile(lens_ref, jnp.minimum(i, total - 1), slots), 0)

    def writes(i, lens_ref):
        return (jnp.minimum(i, 2 * live_blocks(lens_ref, slots) - 1), 0)

    shape = jax.ShapeDtypeStruct((rows, width), BF16)
    return pl.pallas_call(
        kernel,
        out_shape=(shape,) * 4,
        grid_spec=pltpu.PrefetchScalarGridSpec(
            num_scalar_prefetch=1,
            grid=(tiles,),
            in_specs=[
                pl.BlockSpec((TILE, width), reads),
                pl.BlockSpec((TILE, width), reads),
                pl.BlockSpec(vecs.shape, lambda i, lens_ref: (0, 0)),
            ],
            out_specs=[pl.BlockSpec((TILE, width), writes)] * 4,
        ),
        compiler_params=pltpu.CompilerParams(vmem_limit_bytes=VMEM),
        cost_estimate=pl.CostEstimate(
            flops=rows * width * 8, bytes_accessed=rows * width * 12, transcendentals=0
        ),
        name="norm_rows",
    )(lens, layer_input, cotangent, vecs)


class Gathered:
    def __init__(self, pieces, shard):
        self.pieces = [piece for piece, _, _ in pieces]
        self.places = [(mask, extra) for _, mask, extra in pieces]
        self.shard = shard
        self.width = self.pieces[0].shape[1]

    def copies(self, refs, target, sems):
        if self.places[0][0] is not None:
            me = lax.axis_index("dp")
        out = []
        for index, (ref, (mask, extra)) in enumerate(zip(refs, self.places)):
            count = ref.shape[0]
            start = 0 if mask is None else (me ^ mask) * self.shard + extra
            start = start if mask is None else pl.multiple_of(start, count)
            out.append(
                pltpu.make_async_copy(ref, target.at[pl.ds(start, count), :], sems.at[index])
            )
        return out


def any_specs(count):
    return [pl.BlockSpec(memory_space=pl.ANY)] * count


def project_rows(lens, normed, upstream, weights, shift_row, table, slots, qkv_width):
    rows, width = normed.shape
    att_width = weights.width - qkv_width
    blocks = rows // BLOCK
    count = len(weights.pieces)

    def kernel(lens_ref, n_ref, up_ref, shift_ref, table_ref, *rest):
        refs, (qkv_ref, back_ref, held, sems) = rest[:count], rest[count:]
        i = pl.program_id(0)

        @pl.when(i == 0)
        def _():
            copies = weights.copies(refs, held, sems)
            for copy in copies:
                copy.start()
            for copy in copies:
                copy.wait()

        @pl.when(i < live_blocks(lens_ref, slots))
        def _():
            for piece in range(qkv_width // HD):
                cols = slice(piece * HD, (piece + 1) * HD)
                part = jnp.dot(n_ref[...], held[:, cols], preferred_element_type=F32)
                part = part + shift_ref[0:1, cols]
                if piece % 3 == 2:
                    qkv_ref[:, cols] = part.astype(BF16)
                    continue
                for half in range(BLOCK // TILE):
                    tile = slice(half * TILE, (half + 1) * TILE)
                    source = source_tile(lens_ref, i * (BLOCK // TILE) + half, slots)
                    place = pl.multiple_of((source % SLOT_TILES) * TILE, TILE)
                    qkv_ref[tile, cols] = turn(
                        part[tile], table_ref, pl.ds(place, TILE), 1
                    ).astype(BF16)
            back_ref[...] = jnp.dot(
                up_ref[...], held[:, qkv_width:], preferred_element_type=F32
            ).astype(BF16)

    def block(i, lens_ref):
        return (jnp.minimum(i, live_blocks(lens_ref, slots) - 1), 0)

    whole2 = lambda i, lens_ref: (0, 0)
    return pl.pallas_call(
        kernel,
        out_shape=(
            jax.ShapeDtypeStruct((rows, qkv_width), BF16),
            jax.ShapeDtypeStruct((rows, att_width), BF16),
        ),
        grid_spec=pltpu.PrefetchScalarGridSpec(
            num_scalar_prefetch=1,
            grid=(blocks,),
            in_specs=[
                pl.BlockSpec((BLOCK, width), block),
                pl.BlockSpec((BLOCK, width), block),
                pl.BlockSpec(shift_row.shape, whole2),
                pl.BlockSpec(table.shape, lambda i, lens_ref: (0, 0, 0)),
            ]
            + any_specs(count),
            out_specs=[
                pl.BlockSpec((BLOCK, qkv_width), block),
                pl.BlockSpec((BLOCK, att_width), block),
            ],
            scratch_shapes=[
                pltpu.VMEM((width, weights.width), BF16),
                pltpu.SemaphoreType.DMA((count,)),
            ],
        ),
        compiler_params=pltpu.CompilerParams(vmem_limit_bytes=VMEM),
        cost_estimate=pl.CostEstimate(
            flops=2 * rows * width * weights.width,
            bytes_accessed=rows * width * 8,
            transcendentals=0,
        ),
        name="project_rows",
    )(lens, normed, upstream, shift_row, table, *weights.pieces)


def attend(lens, qkv, back, table, slots):
    rows, qkv_width = qkv.shape
    heads = qkv_width // (3 * HD)
    scale = HD ** (-0.5)

    def kernel(lens_ref, qkv_ref, back_ref, table_ref, att_ref, grad_ref, sum_ref, dk_acc, dv_acc):
        slot = pl.program_id(1)
        start = 0
        count = 0
        length = 0
        total = 0
        for other in range(slots):
            own = slot_tiles(lens_ref, other)
            start = jnp.where(other < slot, start + own, start)
            count = jnp.where(other == slot, own, count)
            length = jnp.where(other == slot, lens_ref[other], length)
            total = total + own
        limit = jnp.maximum(length, 1)

        @pl.when(slot == 0)
        def _():
            sum_ref[...] = jnp.zeros_like(sum_ref)
            for index in range(2 * LEAST + 6):
                if index * TILE < rows:
                    dead = (index >= total) & (index < 2 * live_blocks(lens_ref, slots))

                    @pl.when(dead)
                    def _(index=index):
                        tile = slice(index * TILE, (index + 1) * TILE)
                        att_ref[tile, :] = jnp.zeros((TILE, HD), BF16)
                        grad_ref[tile, :] = jnp.zeros((TILE, 3 * HD), BF16)

        base = start * TILE
        dot_nt = lambda a, b: lax.dot_general(
            a, b, (((1,), (1,)), ((), ())), preferred_element_type=F32
        )
        dot_tn = lambda a, b: lax.dot_general(
            a, b, (((0,), (0,)), ((), ())), preferred_element_type=F32
        )

        def keep_sum(value, cols):
            sum_ref[0:1, cols] += jnp.sum(value.astype(F32), axis=0, keepdims=True)

        for i in range(SLOT_TILES):

            @pl.when(count > i)
            def _(i=i):
                span = (i + 1) * TILE
                mine = pl.ds(pl.multiple_of(base + i * TILE, TILE), TILE)
                seen = pl.ds(pl.multiple_of(base, TILE), span)
                query = qkv_ref[mine, 0:HD]
                keys = qkv_ref[seen, HD : 2 * HD]
                values = qkv_ref[seen, 2 * HD : 3 * HD]
                push = back_ref[mine, :]
                place = i * TILE + lax.broadcasted_iota(jnp.int32, (TILE, span), 0)
                column = lax.broadcasted_iota(jnp.int32, (TILE, span), 1)
                allowed = (column <= place) & (column < limit)
                scores = jnp.where(allowed, dot_nt(query, keys) * scale, -1e30)
                powers = jnp.exp(scores - jnp.max(scores, axis=-1, keepdims=True))
                weights = powers / jnp.sum(powers, axis=-1, keepdims=True)
                low = weights.astype(BF16)
                att_ref[mine, :] = jnp.dot(low, values, preferred_element_type=F32).astype(BF16)
                pushed = dot_nt(push, values)
                inner = jnp.sum(weights * pushed, axis=-1, keepdims=True)
                dscores = (weights * (pushed - inner)).astype(BF16)
                dquery = jnp.dot(dscores, keys, preferred_element_type=F32) * scale
                dquery = turn(dquery, table_ref, slice(i * TILE, span), -1).astype(BF16)
                grad_ref[mine, 0:HD] = dquery
                keep_sum(dquery, slice(0, HD))
                dkeys = dot_tn(dscores, query)
                dvalues = dot_tn(low, push)
                if i > 0:
                    dk_acc[0 : i * TILE, :] += dkeys[0 : i * TILE]
                    dv_acc[0 : i * TILE, :] += dvalues[0 : i * TILE]
                dk_acc[i * TILE : span, :] = dkeys[i * TILE : span]
                dv_acc[i * TILE : span, :] = dvalues[i * TILE : span]

        for i in range(SLOT_TILES):

            @pl.when(count > i)
            def _(i=i):
                tile = slice(i * TILE, (i + 1) * TILE)
                mine = pl.ds(pl.multiple_of(base + i * TILE, TILE), TILE)
                dkeys = turn(dk_acc[tile, :] * scale, table_ref, tile, -1).astype(BF16)
                dvalues = dv_acc[tile, :].astype(BF16)
                grad_ref[mine, HD : 2 * HD] = dkeys
                grad_ref[mine, 2 * HD : 3 * HD] = dvalues
                keep_sum(dkeys, slice(HD, 2 * HD))
                keep_sum(dvalues, slice(2 * HD, 3 * HD))

    by_head = lambda h, s, lens_ref: (0, h)
    return pl.pallas_call(
        kernel,
        out_shape=(
            jax.ShapeDtypeStruct((rows, heads * HD), BF16),
            jax.ShapeDtypeStruct((rows, qkv_width), BF16),
            jax.ShapeDtypeStruct((8, qkv_width), F32),
        ),
        grid_spec=pltpu.PrefetchScalarGridSpec(
            num_scalar_prefetch=1,
            grid=(heads, slots),
            in_specs=[
                pl.BlockSpec((rows, 3 * HD), by_head),
                pl.BlockSpec((rows, HD), by_head),
                pl.BlockSpec(table.shape, lambda h, s, lens_ref: (0, 0, 0)),
            ],
            out_specs=[
                pl.BlockSpec((rows, HD), by_head),
                pl.BlockSpec((rows, 3 * HD), by_head),
                pl.BlockSpec((8, 3 * HD), by_head),
            ],
            scratch_shapes=[pltpu.VMEM((SEQ_LEN, HD), F32), pltpu.VMEM((SEQ_LEN, HD), F32)],
        ),
        compiler_params=pltpu.CompilerParams(vmem_limit_bytes=VMEM),
        cost_estimate=pl.CostEstimate(
            flops=14 * heads * slots * SEQ_LEN * SEQ_LEN * HD,
            bytes_accessed=rows * qkv_width * 6,
            transcendentals=heads * slots * SEQ_LEN * SEQ_LEN,
        ),
        name="attend",
    )(lens, qkv, back, table)


def middle(lens, first, span, tensors, vecs, offset_row, entry, expand, shrink, carried, slots):
    normed, upstream, attended, dpacked, inputs = tensors
    rows, width = normed.shape
    hidden_width = expand.width
    qkv_width = dpacked.shape[1]
    att_width = attended.shape[1]
    counts = [len(entry.pieces), len(expand.pieces), len(shrink.pieces)]
    total = sum(counts)
    hold = 2 if carried is not None else 0
    chunk = 512
    nt = (((1,), (1,)), ((), ()))

    def kernel(lens_ref, n_ref, up_ref, att_ref, dp_ref, x_ref, vec_ref, off_ref, *rest):
        refs = rest[:total]
        rest = rest[total + hold :]
        act_ref, dh_ref, both_ref, sum_ref = rest[:4]
        held_e, held_x, held_s, done, sems_e, sems_x, sems_s = rest[4:]
        i = pl.program_id(0)

        def fetch():
            a, b = counts[0], counts[0] + counts[1]
            return (
                expand.copies(refs[a:b], held_x, sems_x),
                shrink.copies(refs[b:], held_s, sems_s),
                entry.copies(refs[:a], held_e, sems_e),
            )

        @pl.when(i == 0)
        def _():
            sum_ref[...] = jnp.zeros_like(sum_ref)
            for group in fetch():
                for copy in group:
                    copy.start()
            for copy in fetch()[0]:
                copy.wait()
            for copy in fetch()[1]:
                copy.wait()

        @pl.when(first + i < live_blocks(lens_ref, slots))
        def _():
            for start in range(0, hidden_width, chunk):
                cols = slice(start, start + chunk)
                hidden = jnp.dot(n_ref[...], held_x[:, cols], preferred_element_type=F32)
                hidden = hidden + off_ref[0:1, cols]
                dact = jnp.dot(up_ref[...], held_s[:, cols], preferred_element_type=F32)
                below = 0.5 + 0.5 * lax.erf(hidden * (0.5**0.5))
                slope = below + hidden * (
                    jnp.exp(-0.5 * hidden * hidden) * ((2.0 * math.pi) ** -0.5)
                )
                act_ref[:, cols] = (hidden * below).astype(BF16)
                dhidden = (dact * slope).astype(BF16)
                dh_ref[:, cols] = dhidden
                sum_ref[5:6, cols] += jnp.sum(dhidden.astype(F32), axis=0, keepdims=True)
        @pl.when(i == 0)
        def _():
            for copy in fetch()[2]:
                copy.wait()

        @pl.when(first + i < live_blocks(lens_ref, slots))
        def _():
            values = x_ref[...].astype(F32)
            centred, scale = norm_parts(values)
            hat = centred * scale
            mean_e = jnp.zeros((BLOCK, 1), F32)
            mean_eh = jnp.zeros((BLOCK, 1), F32)
            for start in range(0, width, chunk):
                cols = slice(start, start + chunk)
                part = lax.dot_general(
                    att_ref[...], held_e[cols, qkv_width:], nt, preferred_element_type=F32
                ) + lax.dot_general(
                    act_ref[...], held_s[cols, :], nt, preferred_element_type=F32
                )
                both_ref[0, :, cols] = part.astype(BF16)
            for start in range(0, width, chunk):
                cols = slice(start, start + chunk)
                two = lax.dot_general(
                    dh_ref[...], held_x[cols, :], nt, preferred_element_type=F32
                )
                one = lax.dot_general(
                    dp_ref[...], held_e[cols, :qkv_width], nt, preferred_element_type=F32
                )
                part = hat[:, cols]
                sum_ref[0:1, cols] += jnp.sum(one * part, axis=0, keepdims=True)
                sum_ref[1:2, cols] += jnp.sum(one, axis=0, keepdims=True)
                sum_ref[2:3, cols] += jnp.sum(two * part, axis=0, keepdims=True)
                sum_ref[3:4, cols] += jnp.sum(two, axis=0, keepdims=True)
                sum_ref[4:5, cols] += jnp.sum(up_ref[:, cols].astype(F32), axis=0, keepdims=True)
                err = one * vec_ref[0:1, cols] + two * vec_ref[2:3, cols]
                done[:, cols] = err
                mean_e = mean_e + jnp.sum(err, axis=-1, keepdims=True)
                mean_eh = mean_eh + jnp.sum(err * part, axis=-1, keepdims=True)
            mean_e = mean_e * (1.0 / width)
            mean_eh = mean_eh * (1.0 / width)
            for start in range(0, width, chunk):
                cols = slice(start, start + chunk)
                both_ref[1, :, cols] = (
                    scale * (done[:, cols] - mean_e - hat[:, cols] * mean_eh)
                ).astype(BF16)

    def block(i, lens_ref):
        return (jnp.minimum(first + i, live_blocks(lens_ref, slots) - 1), 0)

    def local(i, lens_ref):
        top = jnp.maximum(live_blocks(lens_ref, slots) - 1 - first, 0)
        return (0, jnp.minimum(i, top), 0)

    def kept(i, lens_ref):
        top = jnp.maximum(live_blocks(lens_ref, slots) - 1, first)
        return (jnp.minimum(first + i, top), 0)

    whole2 = lambda i, lens_ref: (0, 0)
    sum_width = max(width, hidden_width)
    hidden_shape = jax.ShapeDtypeStruct((rows, hidden_width), BF16)
    args = [lens, normed, upstream, attended, dpacked, inputs, vecs, offset_row]
    args += entry.pieces + expand.pieces + shrink.pieces
    aliases = {}
    if carried is not None:
        aliases = {len(args): 0, len(args) + 1: 1}
        args += list(carried)
    return pl.pallas_call(
        kernel,
        out_shape=(
            hidden_shape,
            hidden_shape,
            jax.ShapeDtypeStruct((2, span * BLOCK, width), BF16),
            jax.ShapeDtypeStruct((8, sum_width), F32),
        ),
        grid_spec=pltpu.PrefetchScalarGridSpec(
            num_scalar_prefetch=1,
            grid=(span,),
            in_specs=[
                pl.BlockSpec((BLOCK, width), block),
                pl.BlockSpec((BLOCK, width), block),
                pl.BlockSpec((BLOCK, att_width), block),
                pl.BlockSpec((BLOCK, qkv_width), block),
                pl.BlockSpec((BLOCK, width), block),
                pl.BlockSpec(vecs.shape, whole2),
                pl.BlockSpec(offset_row.shape, whole2),
            ]
            + any_specs(total + hold),
            out_specs=[
                pl.BlockSpec((BLOCK, hidden_width), kept),
                pl.BlockSpec((BLOCK, hidden_width), kept),
                pl.BlockSpec((2, BLOCK, width), local),
                pl.BlockSpec((8, sum_width), whole2),
            ],
            scratch_shapes=[
                pltpu.VMEM((width, entry.width), BF16),
                pltpu.VMEM((width, expand.width), BF16),
                pltpu.VMEM((width, shrink.width), BF16),
                pltpu.VMEM((BLOCK, width), F32),
                pltpu.SemaphoreType.DMA((counts[0],)),
                pltpu.SemaphoreType.DMA((counts[1],)),
                pltpu.SemaphoreType.DMA((counts[2],)),
            ],
        ),
        input_output_aliases=aliases,
        compiler_params=pltpu.CompilerParams(vmem_limit_bytes=VMEM),
        cost_estimate=pl.CostEstimate(
            flops=2 * span * BLOCK * width * (4 * hidden_width + qkv_width + att_width),
            bytes_accessed=3 * width * hidden_width * 2 + span * BLOCK * width * 16,
            transcendentals=2 * span * BLOCK * hidden_width,
        ),
        name="middle",
    )(*args)


def gradient(lens, pairs, slots, shard, split):
    rows, width = pairs[0][0].shape
    blocks = width // shard
    sizes = [right.shape[1] for _, right in pairs]
    total = sum(sizes)
    half = blocks // 2
    most = rows // BLOCK

    def kernel(lens_ref, *rest):
        lefts = rest[: len(pairs)]
        rights = rest[len(pairs) : 2 * len(pairs)]
        outs = rest[2 * len(pairs) :]
        j = pl.program_id(0)
        live = live_blocks(lens_ref, slots)

        def emit(ref, depth):
            start = 0
            for left, right, size in zip(lefts, rights, sizes):
                ref[0, :, start : start + size] = lax.dot_general(
                    left[: depth * BLOCK, :],
                    right[: depth * BLOCK, :],
                    (((0,), (0,)), ((), ())),
                    preferred_element_type=F32,
                ).astype(BF16)
                start += size

        for depth in range(LEAST, most + 1):
            match = live == depth
            if split:
                for which, ref in enumerate(outs):
                    here = (j >= half) if which else (j < half)

                    @pl.when(match & here)
                    def _(ref=ref, depth=depth):
                        emit(ref, depth)

            else:

                @pl.when(match)
                def _(depth=depth):
                    emit(outs[0], depth)

    def left_block(j, lens_ref):
        if not split:
            return (0, j)
        mask = jnp.where(j < half, 2 * j + 1, 2 * (j - half))
        return (0, lens_ref[slots] ^ mask)

    whole2 = lambda j, lens_ref: (0, 0)
    if split:
        out_shape = [jax.ShapeDtypeStruct((half, shard, total), BF16)] * 2
        out_specs = [
            pl.BlockSpec((1, shard, total), lambda j, lens_ref: (jnp.minimum(j, half - 1), 0, 0)),
            pl.BlockSpec((1, shard, total), lambda j, lens_ref: (jnp.maximum(j - half, 0), 0, 0)),
        ]
    else:
        out_shape = [jax.ShapeDtypeStruct((blocks, shard, total), BF16)]
        out_specs = [pl.BlockSpec((1, shard, total), lambda j, lens_ref: (j, 0, 0))]
    return pl.pallas_call(
        kernel,
        out_shape=out_shape,
        grid_spec=pltpu.PrefetchScalarGridSpec(
            num_scalar_prefetch=1,
            grid=(blocks,),
            in_specs=[pl.BlockSpec((rows, shard), left_block) for _ in pairs]
            + [pl.BlockSpec(right.shape, whole2) for _, right in pairs],
            out_specs=out_specs,
        ),
        compiler_params=pltpu.CompilerParams(vmem_limit_bytes=VMEM),
        cost_estimate=pl.CostEstimate(
            flops=2 * rows * width * total,
            bytes_accessed=rows * (width + total) * 2 + width * total * 2,
            transcendentals=0,
        ),
        name="gradient",
    )(lens, *[left for left, _ in pairs], *[right for _, right in pairs])


def finish_rows(lens, layer_input, cotangent, summed, bias_row, slots):
    rows = layer_input.shape[0]
    width = summed.shape[2]
    tiles = rows // TILE

    def kernel(lens_ref, x_ref, cot_ref, sum_ref, bias_ref, out_ref, grad_ref):
        i = pl.program_id(0)
        target = compact_tile(lens_ref, i, slots)

        @pl.when(target >= 0)
        def _():
            length = lens_ref[i // SLOT_TILES]
            place = (i % SLOT_TILES) * TILE + lax.broadcasted_iota(jnp.int32, (TILE, 1), 0)
            live = place < length
            total = x_ref[...].astype(F32) + sum_ref[0].astype(F32) + bias_ref[0:1, :]
            out_ref[...] = jnp.where(live, total, 0.0).astype(BF16)
            grad = cot_ref[...].astype(F32) + sum_ref[1].astype(F32)
            grad_ref[...] = jnp.where(live, grad, 0.0).astype(BF16)

        @pl.when(target < 0)
        def _():
            out_ref[...] = jnp.zeros_like(out_ref)
            grad_ref[...] = jnp.zeros_like(grad_ref)

    def own(i, lens_ref):
        return (i, lens_ref[slots + 1])

    def packed(i, lens_ref):
        return (0, jnp.maximum(compact_tile(lens_ref, i, slots), 0), 0)

    shape = jax.ShapeDtypeStruct((rows, width), BF16)
    return pl.pallas_call(
        kernel,
        out_shape=(shape, shape),
        grid_spec=pltpu.PrefetchScalarGridSpec(
            num_scalar_prefetch=1,
            grid=(tiles,),
            in_specs=[
                pl.BlockSpec((TILE, width), own),
                pl.BlockSpec((TILE, width), own),
                pl.BlockSpec((2, TILE, width), packed),
                pl.BlockSpec(bias_row.shape, lambda i, lens_ref: (0, 0)),
            ],
            out_specs=[pl.BlockSpec((TILE, width), lambda i, lens_ref: (i, 0))] * 2,
        ),
        cost_estimate=pl.CostEstimate(
            flops=rows * width * 4, bytes_accessed=rows * width * 12, transcendentals=0
        ),
        name="finish_rows",
    )(lens, layer_input, cotangent, summed, bias_row)


def adamw(master, moments, gradient):
    first_moment = beta_one * moments[0] + (1.0 - beta_one) * gradient
    root_moment = jnp.sqrt(
        beta_two * moments[1] * moments[1] + (1.0 - beta_two) * gradient * gradient
    )
    first_hat = first_moment / (1.0 - beta_one**STEP)
    root_hat = root_moment / math.sqrt(1.0 - beta_two**STEP)
    update = -learn_rate * (first_hat / (root_hat + adam_eps) + decay_rate * master)
    return (jnp.stack([first_moment, root_moment]), update)


def exchange(values, spread, name, key):
    dp, tensor = lax.axis_size("dp"), lax.axis_size("tensor")
    count = dp * tensor
    shape = values.shape if spread else values.shape[1:]

    def kernel(x_ref, out_ref, send_sems, recv_sems):
        me = lax.axis_index("dp") * tensor + lax.axis_index("tensor")
        barrier = pltpu.get_barrier_semaphore()

        def place(step):
            other = lax.rem(me + step, count)
            return other, (other // tensor, lax.rem(other, tensor))

        @pl.loop(1, count)
        def _(step):
            _, target = place(step)
            pl.semaphore_signal(barrier, inc=1, device_id=target, device_id_type=MESH)

        pl.semaphore_wait(barrier, count - 1)

        def copy(step):
            other, target = place(step)
            return pltpu.make_async_remote_copy(
                src_ref=x_ref if spread else x_ref.at[other],
                dst_ref=out_ref.at[me],
                send_sem=send_sems.at[step],
                recv_sem=recv_sems.at[step],
                device_id=target,
                device_id_type=MESH,
            )

        @pl.loop(1, count)
        def _(step):
            copy(step).start()

        out_ref[me] = x_ref[...] if spread else x_ref[me]

        @pl.loop(1, count)
        def _(step):
            copy(step).wait()

    return pl.pallas_call(
        kernel,
        out_shape=jax.ShapeDtypeStruct((count, *shape), values.dtype),
        in_specs=[pl.BlockSpec(memory_space=pltpu.VMEM)],
        out_specs=pl.BlockSpec(memory_space=pltpu.VMEM),
        scratch_shapes=[pltpu.SemaphoreType.DMA((count,)), pltpu.SemaphoreType.DMA((count,))],
        compiler_params=pltpu.CompilerParams(collective_id=key, has_side_effects=True),
        name=name,
    )(values)


def gather_cube(own, key):
    shard, width = own.shape
    parts = 4
    step = shard // parts
    orders = {2: (0, 1, 2, 3), 4: (2, 3, 0, 1)}

    def kernel(own_ref, out_ref, keep_sem, send_sems, recv_sems):
        me = lax.axis_index("dp")
        barrier = pltpu.get_barrier_semaphore()
        for mask in (1, 2, 4):
            pl.semaphore_signal(
                barrier, inc=1, device_id={"dp": me ^ mask}, device_id_type=MESH
            )
        pl.semaphore_wait(barrier, 3)

        def rows(mask, part, count=1):
            start = pl.multiple_of((me ^ mask) * shard + part * step, step)
            return out_ref.at[pl.ds(start, count * step), :]

        slot = iter(range(64))

        def send(source, target, mask):
            index = next(slot)
            copy = pltpu.make_async_remote_copy(
                src_ref=source,
                dst_ref=target,
                send_sem=send_sems.at[index],
                recv_sem=recv_sems.at[index],
                device_id={"dp": me ^ mask},
                device_id_type=MESH,
            )
            copy.start()
            return copy

        keep = pltpu.make_async_copy(own_ref, rows(0, 0, parts), keep_sem)
        first = {}
        for turn_ in range(parts):
            for mask in (2, 4):
                part = orders[mask][turn_]
                piece = own_ref.at[pl.ds(part * step, step), :]
                first[mask, part] = send(piece, rows(0, part), mask)
        late = [send(own_ref, rows(0, 0, parts), 1)]
        keep.start()
        second = []
        for turn_ in range(parts):
            for mask in (2, 4):
                part = orders[mask][turn_]
                first[mask, part].wait_recv()
                piece = rows(mask, part)
                late.append(send(piece, piece, 1))
                if turn_ < parts // 2:
                    second.append((6, part, send(piece, piece, 6 ^ mask)))
        for mask, part, copy in second:
            copy.wait_recv()
            piece = rows(mask, part)
            late.append(send(piece, piece, 1))
        keep.wait()
        for copy in late:
            copy.wait()
        for copy in first.values():
            copy.wait_send()
        for _, _, copy in second:
            copy.wait_send()

    sems = 64
    return pl.pallas_call(
        kernel,
        out_shape=jax.ShapeDtypeStruct((8 * shard, width), own.dtype),
        in_specs=[pl.BlockSpec(memory_space=pltpu.VMEM)],
        out_specs=pl.BlockSpec(memory_space=pl.ANY),
        scratch_shapes=[
            pltpu.SemaphoreType.DMA,
            pltpu.SemaphoreType.DMA((sems,)),
            pltpu.SemaphoreType.DMA((sems,)),
        ],
        compiler_params=pltpu.CompilerParams(collective_id=key, has_side_effects=True),
        name="gather_cube",
    )(own)


def swap(values, mask):
    size = lax.axis_size("dp")
    return lax.ppermute(values, "dp", [(i, i ^ mask) for i in range(size)])


def after(values, *others):
    return lax.optimization_barrier((values, others))[0]


def whole(full, shard):
    return Gathered([(full, None, 0)], shard)


def gather_plain(own):
    return lax.all_gather(own, "dp", axis=0, tiled=True)


def reduce_plain(parts):
    return lax.psum_scatter(parts[0], "dp", scatter_dimension=0, tiled=True)[0].astype(F32)


def reduce_cube(parts):
    other, own = parts
    half = own.shape[1] // 2
    up = lambda v: v.astype(F32)
    got = swap(other, 1)
    send_x = (up(own[1::2, :half]) + up(got[1::2, :half])).astype(BF16)
    send_y = (up(own[2:, half:]) + up(got[2:, half:])).astype(BF16)
    from_x, from_y = swap(send_x, 2), swap(send_y, 4)
    next_y = (up(own[2, :half]) + up(got[2, :half]) + up(from_x[1])).astype(BF16)
    next_x = (up(own[1, half:]) + up(got[1, half:]) + up(from_y[1])).astype(BF16)
    last_y, last_x = swap(next_y, 4), swap(next_x, 2)
    mine = up(own[0]) + up(got[0])
    return mine + jnp.concatenate([up(from_x[0]) + up(last_y), up(from_y[0]) + up(last_x)], axis=0)


def on_device(
    layer_input,
    cotangent,
    lengths,
    projector,
    projector_moments,
    shifts,
    shifts_moments,
    combiner,
    combiner_moments,
    expander,
    expander_moments,
    offsets,
    offsets_moments,
    reducer,
    reducer_moments,
    vectors,
    vectors_moments,
):
    dp, tensor = lax.axis_size("dp"), lax.axis_size("tensor")
    rank, lane = lax.axis_index("dp"), lax.axis_index("tensor")
    slots = lengths.shape[0]
    rows, width = layer_input.shape
    shard = projector.shape[0]
    qkv_width = projector.shape[1]
    att_width = combiner.shape[0]
    hidden_width = expander.shape[1]
    lens = jnp.concatenate(
        [lengths, jnp.stack([rank, lane]).astype(jnp.int32), jnp.zeros((3,), jnp.int32)]
    )
    table = rotary_tables()

    entry_own = jnp.concatenate([projector.astype(BF16), combiner.astype(BF16).T], axis=1)
    expand_own = expander.astype(BF16)
    shrink_own = reducer.astype(BF16).T

    cube = dp == 8
    sizes = [vectors.size, shifts.size, offsets.size]
    small = jnp.concatenate([vectors.reshape(-1), shifts.reshape(-1), offsets.reshape(-1)])
    small = small.astype(BF16).astype(F32)
    small = jnp.pad(small, (0, -small.size % 1024)).reshape(-1, 128)
    small = exchange(small, True, "spread_small", 1).reshape(dp * tensor, -1)
    full_vectors = (
        small[:, : sizes[0]].reshape(dp * tensor, *vectors.shape).transpose(1, 0, 2).reshape(6, -1)
    )
    biases = lax.dynamic_index_in_dim(
        small.reshape(dp, tensor, -1), lane, axis=1, keepdims=False
    )
    shift_row = (
        biases[:, sizes[0] : sizes[0] + sizes[1]]
        .reshape(dp, *shifts.shape)
        .transpose(1, 0, 2)
        .reshape(1, -1)
    )
    offset_row = (
        biases[:, sizes[0] + sizes[1] : sum(sizes)]
        .reshape(dp, *offsets.shape)
        .transpose(1, 0, 2)
        .reshape(1, -1)
    )
    vecs = jnp.pad(full_vectors, ((0, 2), (0, 0)))

    entry = whole(gather_cube(entry_own, 2) if cube else gather_plain(entry_own), shard)
    expand = whole(gather_plain(expand_own), shard)
    shrink = whole(gather_plain(shrink_own), shard)
    reduce_parts = reduce_cube if cube else reduce_plain

    normed_one, normed_two, inputs, upstream = norm_rows(lens, layer_input, cotangent, vecs, slots)
    qkv, back = project_rows(
        lens, normed_one, upstream, entry, shift_row, table, slots, qkv_width
    )
    attended, dpacked, shift_sum = attend(lens, qkv, back, table, slots)
    split = cube
    entry_parts = gradient(lens, [(normed_one, dpacked), (upstream, attended)], slots, shard, split)

    blocks = rows // BLOCK
    tensors = (normed_two, upstream, attended, dpacked, inputs)
    mid_lens = after(lens, *entry_parts)
    carried = None
    sums = 0.0
    reduced = []
    first = 0
    for span in (1, 2, blocks - 3):
        act, dhid, both, part = middle(
            mid_lens, first, span, tensors, vecs, offset_row, entry, expand, shrink, carried, slots
        )
        carried = (act, dhid)
        sums = sums + part
        first += span
        reduced.append(
            lax.psum_scatter(both, "tensor", scatter_dimension=2, tiled=True)
        )
    shrink_parts = gradient(lens, [(upstream, act)], slots, shard, split)
    expand_parts = gradient(lens, [(normed_two, dhid)], slots, shard, split)

    entry_share = reduce_parts(entry_parts)
    shrink_share = reduce_parts(shrink_parts)
    expand_share = reduce_parts(expand_parts)
    projector_grad = entry_share[:, :qkv_width]
    combiner_grad = entry_share[:, qkv_width:].T
    reducer_grad = shrink_share.T
    expander_grad = expand_share

    shift_part = shift_sum[0].reshape(shifts.shape[0], dp, -1).transpose(1, 0, 2).reshape(dp, 1, -1)
    offset_part = sums[5, :hidden_width].reshape(offsets.shape[0], dp, -1)
    offset_part = offset_part.transpose(1, 0, 2).reshape(dp, 1, -1)
    norm_part = sums[:4, :width].reshape(4, dp, tensor, -1).transpose(1, 2, 0, 3)
    bias_part = sums[4, :width].reshape(dp, tensor, -1)
    alike = jnp.concatenate(
        [
            bias_part,
            jnp.broadcast_to(shift_part, (dp, tensor, shifts.size)),
            jnp.broadcast_to(offset_part, (dp, tensor, offsets.size)),
        ],
        axis=2,
    )
    alike = jnp.where(jnp.arange(tensor)[None, :, None] == lane, alike, 0.0)
    packed = jnp.concatenate([norm_part.reshape(dp, tensor, -1), alike], axis=2)
    used = packed.shape[2]
    packed = jnp.pad(packed, ((0, 0), (0, 0), (0, -used % 1024)))
    packed = exchange(packed.reshape(dp * tensor, -1, 128), False, "sum_small", 3)
    packed = jnp.sum(packed, axis=0).reshape(-1)
    marks = [4 * vectors.shape[1], vectors.shape[1], shifts.size, offsets.size]
    marks = [sum(marks[:k]) for k in range(5)]
    norm_grad, bias_grad, shifts_grad, offsets_grad = (
        packed[low:high] for low, high in zip(marks, marks[1:])
    )
    shifts_grad = shifts_grad.reshape(shifts.shape)
    offsets_grad = offsets_grad.reshape(offsets.shape)
    bias_grad = bias_grad.reshape(1, -1)
    vectors_grad = jnp.concatenate([norm_grad.reshape(4, -1), bias_grad, bias_grad], axis=0)

    own_width = reduced[0].shape[2]
    own_bias = lax.dynamic_slice_in_dim(
        full_vectors[4] + full_vectors[5], lane * own_width, own_width, 0
    ).reshape(1, -1)
    layer_output, input_gradient = finish_rows(
        lens, layer_input, cotangent, jnp.concatenate(reduced, axis=1), own_bias, slots
    )

    results = [layer_output, input_gradient]
    for master, moments, grad in (
        (projector, projector_moments, projector_grad),
        (shifts, shifts_moments, shifts_grad),
        (combiner, combiner_moments, combiner_grad),
        (expander, expander_moments, expander_grad),
        (offsets, offsets_moments, offsets_grad),
        (reducer, reducer_moments, reducer_grad),
        (vectors, vectors_moments, vectors_grad),
    ):
        states, update = adamw(master, moments, grad)
        results += [grad, states, update]
    return tuple(results)


def solution(mesh):
    rows = P("dp", "tensor")
    cols = P("tensor", "dp")
    deep_rows = P(None, "dp", "tensor")
    deep_cols = P(None, "tensor", "dp")
    both = P(None, ("dp", "tensor"))
    deep_both = P(None, None, ("dp", "tensor"))
    placed = (P("dp", None), P("dp", None), P("dp"))
    results = (rows, rows)
    for plain, deep in (
        (rows, deep_rows),
        (cols, deep_cols),
        (cols, deep_cols),
        (rows, deep_rows),
        (cols, deep_cols),
        (cols, deep_cols),
        (both, deep_both),
    ):
        placed += (plain, deep)
        results += (plain, deep, plain)
    return jax.shard_map(
        on_device, mesh=mesh, in_specs=placed, out_specs=results, check_vma=False
    )
```
